32 devices in a mesh: row: 4 (over z), col: 8 (over y, x, core).
Axes of the slice: x: 2, y: 2, z: 4, core: 2. Of those that a mesh axis runs over, the one named last changes fastest.
Arguments:
- tiles: bfloat16 [4, 8, 128, 128, 128], P('row', 'col'), may hold values from -6 to 6
- tile_row: int32 [4, 8, 128], P('row', 'col'), may hold values from 0 to 63, as said below
- tile_col: int32 [4, 8, 128], P('row', 'col'), may hold values from 0 to 31
- tile_count: int32 [4, 8], P('row', 'col'), may hold values from 16 to 128, as said below
- query_ids: int32 [128], replicated, may hold values from 0 to 32767
- damping: float32 [128], replicated, may hold values from 0.006629126 to 0.026516505
Outputs:
- scores: float32 [32768, 128], P(('row', 'col'))
The draws below stay inside these ranges and needn't reach their ends.
Inputs may be any that keep to these rules, and one draw needn't show every extreme that they name: `tile_count`: some device holds exactly 128 live slots; slots at or past the count hold arbitrary finite values and are ignored. `tile_row`: positions may repeat within a device; such tiles add. For every device and every col index o, the live slots name at most 4 distinct values among o * 8 to o * 8 + 7, and every device reaches 4 for some o. `query_ids`: ids may repeat.
All inputs are finite; a program needn't handle non-finite values.
Results may differ from the reference program's by a relative error of at most 0.003.
Values may be sent and summed in bfloat16 or wider, within the bound.
A program may use at most 128 MiB of HBM per device.

```python
import math
import jax
import jax.numpy as jnp
from jax import lax

TILE = 128
BPD = 8
TILES_DEV = 128
QUERIES = 128
TERMS = 4
TOUCH = 4
NBLK = 256
NODES = 32768
N_ROW = 4
N_COL = 8


def draw_tile_count(key, part):
    shifts = jax.random.randint(key, (N_ROW * N_COL,), 0, 4)
    counts = jnp.right_shift(jnp.full((N_ROW * N_COL,), TILES_DEV, jnp.int32), shifts.astype(jnp.int32))
    fullest = jax.random.randint(jax.random.fold_in(key, 7), (), 0, N_ROW * N_COL)
    counts = counts.at[fullest].set(TILES_DEV)
    return counts.reshape(N_ROW, N_COL).astype(jnp.int32)


def draw_tile_row(key, part):
    devs = N_ROW * N_COL
    owners = jax.random.randint(jax.random.fold_in(key, 11), (devs, TILES_DEV), 0, N_COL)
    starts = jax.random.randint(jax.random.fold_in(key, 12), (devs, N_COL), 0, BPD)
    offsets = jax.random.randint(jax.random.fold_in(key, 13), (devs, TILES_DEV), 0, TOUCH)
    favoured = jax.random.randint(jax.random.fold_in(key, 14), (devs,), 0, N_COL)
    slot = jnp.arange(TILES_DEV, dtype=jnp.int32)
    first = slot < TOUCH
    owners = jnp.where(first[None, :], favoured[:, None], owners)
    offsets = jnp.where(first[None, :], slot[None, :], offsets)
    chosen = jnp.take_along_axis(starts, owners, axis=1)
    local = (chosen + offsets) % BPD
    return (owners * BPD + local).reshape(N_ROW, N_COL, TILES_DEV).astype(jnp.int32)


def with_ends(array, stream_key, low, top_value):
    longest = array.shape.index(max(array.shape))
    spots = []
    for shift in (0, 1):
        where = [jax.random.randint(jax.random.fold_in(stream_key, axis), (), 0, length) for axis, length in enumerate(array.shape)]
        where[longest] = (where[longest] + shift) % array.shape[longest]
        spots.append(tuple(where))
    return array.at[spots[0]].set(low).at[spots[1]].set(top_value)


def levels(key, extent, pieces, least, largest):
    loudness, own = 1.0, jax.random.fold_in(key, 6)
    for dim, shards_of in pieces:
        steps = jnp.exp(jax.random.uniform(jax.random.fold_in(own, dim), (shards_of,), jnp.float32, least / len(pieces), largest / len(pieces)))
        loudness = loudness * jnp.repeat(steps, extent[dim] // shards_of).reshape([-1 if axis == dim else 1 for axis in range(len(extent))])
    return loudness


def normal_values(key, extent, scale, bound, cuts=(), kind=jnp.bfloat16):
    entries = scale * jax.random.normal(key, extent, jnp.float32)
    if cuts:
        entries = entries * levels(key, extent, cuts, -0.22, 0.18)
    return jnp.clip(entries, -bound, bound).astype(kind)


def setup_inputs(seed: int = 0) -> dict:
    keys = jax.random.split(jax.random.key(seed), 7)
    return {
        "tiles": normal_values(keys[0], (N_ROW, N_COL, TILES_DEV, TILE, TILE), 1.0, 6.0, ((0, 4), (1, 8))),
        "tile_row": draw_tile_row(jax.random.fold_in(keys[6], 71), 0),
        "tile_col": with_ends(jax.random.randint(keys[2], (N_ROW, N_COL, TILES_DEV), 0, BPD * N_ROW), jax.random.fold_in(keys[2], 1), 0, (BPD * N_ROW) - 1).astype(jnp.int32),
        "tile_count": draw_tile_count(jax.random.fold_in(keys[6], 71), 0),
        "query_ids": with_ends(jax.random.randint(keys[4], (QUERIES,), 0, NODES), jax.random.fold_in(keys[4], 1), 0, NODES - 1).astype(jnp.int32),
        "damping": jnp.clip(jnp.exp(jax.random.uniform(keys[5], (QUERIES,), jnp.float32, math.log(0.006629126), math.log(0.026516505))), 0.006629126, 0.026516505),
    }


def device_partial(tile_block, rows, cols, count, xcol):
    picked = xcol[cols]
    prod = jnp.einsum("tab,tbq->taq", tile_block.astype(jnp.float32), picked.astype(jnp.float32))
    live = (jnp.arange(tile_block.shape[0], dtype=jnp.int32) < count).astype(jnp.float32)
    prod = prod * live[:, None, None]
    return jax.ops.segment_sum(prod, rows, num_segments=BPD * N_COL)


def reference(tiles, tile_row, tile_col, tile_count, query_ids, damping):
    nodes = NBLK * TILE
    queries = query_ids.shape[0]
    node_ids = jnp.arange(nodes, dtype=jnp.int32)
    xvec = (node_ids[:, None] == query_ids[None, :]).astype(jnp.bfloat16)
    scores = jnp.zeros((nodes, queries), jnp.float32)
    coef = jnp.ones((queries,), jnp.float32)
    for step in range(TERMS):
        xgrid = xvec.reshape(N_ROW, N_COL, BPD, TILE, queries)

        def one_row(ridx):
            def add_col(cidx, total):
                xcol = lax.dynamic_index_in_dim(xgrid, cidx, 1, keepdims=False)
                xcol = xcol.reshape(N_ROW * BPD, TILE, queries)
                tblock = tiles[ridx, cidx]
                part = device_partial(tblock, tile_row[ridx, cidx], tile_col[ridx, cidx], tile_count[ridx, cidx], xcol)
                rounded = lax.optimization_barrier(part.astype(jnp.bfloat16))
                return total + rounded.astype(jnp.float32)

            start = jnp.zeros((BPD * N_COL, TILE, queries), jnp.float32)
            return lax.fori_loop(0, N_COL, add_col, start)

        ysum = lax.map(one_row, jnp.arange(N_ROW, dtype=jnp.int32))
        ysum = ysum.reshape(nodes, queries)
        scores = scores + coef[None, :] * ysum
        coef = coef * damping
        xvec = ysum.astype(jnp.bfloat16)
    return scores
```

```python
import functools

import jax
import jax.numpy as jnp
from jax import lax
from jax.experimental import pallas as pl
from jax.experimental.pallas import tpu as pltpu
from jax.sharding import PartitionSpec as P

BPD = 8
TERMS = 4
TOUCH = 4
HALVES = 2
UNROLL = 8
MESH = pl.DeviceIdType.MESH


def plan(rows, cols, count, n_col, me_col):
    slots = rows.shape[0]
    row_blocks = BPD * n_col
    slot = jnp.arange(slots, dtype=jnp.int32)
    key = jnp.where(slot < count, rows, row_blocks)
    before = (key[None, :] < key[:, None]) | ((key[None, :] == key[:, None]) & (slot[None, :] < slot[:, None]))
    rank = jnp.sum(before.astype(jnp.int32), axis=1)
    at = (rank[None, :] == slot[:, None]).astype(jnp.int32)
    perm = jnp.sum(at * slot[None, :], axis=1)
    scol = jnp.sum(at * cols[None, :], axis=1)
    same = (key[None, :] == key[:, None]) & (slot[None, :] < slot[:, None])
    cont_of = jnp.any(same, axis=1).astype(jnp.int32)
    cont = jnp.sum(at * cont_of[None, :], axis=1)
    blocks = jnp.arange(row_blocks, dtype=jnp.int32)
    hits = key[None, :] == blocks[:, None]
    marked = jnp.any(hits, axis=1).reshape(n_col, BPD)
    last = (jnp.sum((key[None, :] <= blocks[:, None]).astype(jnp.int32), axis=1) - 1).reshape(n_col, BPD)
    local = jnp.arange(BPD, dtype=jnp.int32)
    earlier = marked[:, None, :] & (local[None, None, :] < local[None, :, None])
    place = jnp.sum(earlier.astype(jnp.int32), axis=2)
    places = jnp.arange(TOUCH, dtype=jnp.int32)
    select = marked[:, None, :] & (place[:, None, :] == places[None, :, None])
    ends = jnp.sum(select.astype(jnp.int32) * last[:, None, :], axis=2).reshape(n_col * TOUCH)
    pos = jnp.where(marked, me_col * TOUCH + place, n_col * TOUCH)
    pos = jnp.pad(pos, ((0, 0), (0, 128 - BPD))).reshape(n_col, 1, 128)
    return perm, scol, cont, ends, pos


def katz_kernel(
    n_row, n_col,
    perm, scol, cont, ends,
    pos_ref, qid_ref, damp_ref, tiles_hbm,
    out_ref,
    tiles, run, send, got, xbuf, total, coef, posbuf, pos_smem,
    tile_sem, pos_send, pos_recv, local_sem, send_sem, recv_sem, xsend_sem, xrecv_sem,
):
    me_r = lax.axis_index("row")
    me_c = lax.axis_index("col")
    slots, tile, _ = tiles.shape
    queries = qid_ref.shape[1]
    width = queries // HALVES

    load = pltpu.make_async_copy(tiles_hbm, tiles, tile_sem)
    load.start()
    barrier = pltpu.get_barrier_semaphore()
    for d in range(1, n_col):
        pl.semaphore_signal(barrier, inc=1, device_id=(me_r, lax.rem(me_c + d, n_col)), device_id_type=MESH)
    for d in range(1, n_row):
        pl.semaphore_signal(barrier, inc=1, device_id=(lax.rem(me_r + d, n_row), me_c), device_id_type=MESH)

    lane = lax.broadcasted_iota(jnp.int32, (queries, tile), 1)
    qid = jnp.transpose(jnp.broadcast_to(qid_ref[...], (tile, queries))) - lane
    coef[...] = jnp.transpose(jnp.broadcast_to(damp_ref[...], (tile, queries)))

    def first_x(j, carry):
        base = ((j // BPD * n_col + me_c) * BPD + lax.rem(j, BPD)) * tile
        hot = jnp.where(qid == base, 1.0, 0.0).astype(jnp.bfloat16)
        for h in range(HALVES):
            xbuf[h][j] = hot[h * width:(h + 1) * width]
        return carry

    lax.fori_loop(0, n_row * BPD, first_x, 0)
    for t in range(TERMS * HALVES):
        got[t][n_col * TOUCH] = jnp.zeros((width, tile), jnp.bfloat16)
    load.wait()

    def compute(t):
        def body(i, acc):
            for u in range(UNROLL):
                p = i * UNROLL + u
                prod = lax.dot_general(
                    xbuf[t][scol[p]], tiles[perm[p]], (((1,), (1,)), ((), ())), preferred_element_type=jnp.float32
                )
                acc = jnp.where(cont[p] > 0, acc, 0.0) + prod
                run[p] = acc.astype(jnp.bfloat16)
            return acc

        lax.fori_loop(0, slots // UNROLL, body, jnp.zeros((width, tile), jnp.float32))

        def pack(s, carry):
            send[t, s] = run[ends[s]]
            return carry

        lax.fori_loop(0, n_col * TOUCH, pack, 0, unroll=4)
        for j in range(TOUCH):
            got[t][me_c * TOUCH + j] = run[ends[me_c * TOUCH + j]]

    def part_copy(t, d):
        peer = lax.rem(me_c + d, n_col)
        return pltpu.make_async_remote_copy(
            src_ref=send.at[t, pl.ds(peer * TOUCH, TOUCH)],
            dst_ref=got[t].at[pl.ds(me_c * TOUCH, TOUCH)],
            send_sem=send_sem.at[t, d], recv_sem=recv_sem.at[t, d],
            device_id=(me_r, peer), device_id_type=MESH,
        )

    def x_copy(t, d):
        mine = pl.ds(me_r * BPD, BPD)
        return pltpu.make_async_remote_copy(
            src_ref=xbuf[t + HALVES].at[mine], dst_ref=xbuf[t + HALVES].at[mine],
            send_sem=xsend_sem.at[t, d], recv_sem=xrecv_sem.at[t, d],
            device_id=(lax.rem(me_r + d, n_row), me_c), device_id_type=MESH,
        )

    def pos_copy(d):
        peer = lax.rem(me_c + d, n_col)
        return pltpu.make_async_remote_copy(
            src_ref=pos_ref.at[peer], dst_ref=posbuf.at[me_c],
            send_sem=pos_send.at[d], recv_sem=pos_recv.at[d],
            device_id=(me_r, peer), device_id_type=MESH,
        )

    def gather_wait(t):
        for d in range(1, n_row):
            x_copy(t, d).wait_recv()

    def reduce(t):
        k, h = divmod(t, HALVES)
        for d in range(1, n_col):
            part_copy(t, d).wait_recv()
        part = pl.ds(h * width, width)
        weight = coef[part, :]
        scale = weight
        for _ in range(k - 1):
            scale = scale * weight

        def block(b, carry):
            acc = got[t][pos_smem[0, 0, b]].astype(jnp.float32)
            for s in range(1, n_col):
                acc = acc + got[t][pos_smem[s, 0, b]].astype(jnp.float32)
            if k == 0:
                total[b, part, :] = acc
            else:
                total[b, part, :] = total[b, part, :] + scale * acc
            if k + 1 < TERMS:
                xbuf[t + HALVES][me_r * BPD + b] = acc.astype(jnp.bfloat16)
            return carry

        lax.fori_loop(0, BPD, block, 0)
        if k + 1 < TERMS:
            for d in range(1, n_row):
                x_copy(t, d).start()

    steps = TERMS * HALVES
    for t in range(steps + 1):
        if t < steps:
            if t >= HALVES:
                gather_wait(t - HALVES)
            compute(t)
            if t == 0:
                pl.semaphore_wait(barrier, n_col - 1 + n_row - 1)
                for d in range(1, n_col):
                    pos_copy(d).start()
            for d in range(1, n_col):
                part_copy(t, d).start()
            if t == 0:
                own = pltpu.make_async_copy(pos_ref.at[me_c], posbuf.at[me_c], local_sem)
                own.start()
                own.wait()
                for d in range(1, n_col):
                    pos_copy(d).wait_recv()
                spill = pltpu.make_async_copy(posbuf, pos_smem, local_sem)
                spill.start()
                spill.wait()
        if t >= 1:
            reduce(t - 1)

    for b in range(BPD):
        out_ref[pl.ds(b * tile, tile), :] = jnp.transpose(total[b])
    for d in range(1, n_col):
        pos_copy(d).wait_send()
        for t in range(steps):
            part_copy(t, d).wait_send()
    for d in range(1, n_row):
        for t in range(steps - HALVES):
            x_copy(t, d).wait_send()


def shards(tiles, tile_row, tile_col, tile_count, query_ids, damping):
    tile_block = tiles[0, 0]
    slots, tile, _ = tile_block.shape
    queries = query_ids.shape[0]
    n_row = lax.axis_size("row")
    n_col = lax.axis_size("col")
    me_col = lax.axis_index("col")
    perm, scol, cont, ends, pos = plan(tile_row[0, 0], tile_col[0, 0], tile_count[0, 0], n_col, me_col)
    width = queries // HALVES
    steps = TERMS * HALVES
    bf16 = jnp.bfloat16
    dma = pltpu.SemaphoreType.DMA
    smem = pl.BlockSpec(memory_space=pltpu.SMEM)
    vmem = pl.BlockSpec(memory_space=pltpu.VMEM)
    return pl.pallas_call(
        functools.partial(katz_kernel, n_row, n_col),
        out_shape=jax.ShapeDtypeStruct((BPD * tile, queries), jnp.float32),
        in_specs=[smem] * 4 + [vmem] * 3 + [pl.BlockSpec(memory_space=pl.ANY)],
        out_specs=vmem,
        scratch_shapes=[
            pltpu.VMEM((slots, tile, tile), bf16),
            pltpu.VMEM((slots, width, tile), bf16),
            pltpu.VMEM((steps, n_col * TOUCH, width, tile), bf16),
            [pltpu.VMEM((n_col * TOUCH + 1, width, tile), bf16)] * steps,
            [pltpu.VMEM((n_row * BPD, width, tile), bf16)] * steps,
            pltpu.VMEM((BPD, queries, tile), jnp.float32),
            pltpu.VMEM((queries, tile), jnp.float32),
            pltpu.VMEM((n_col, 1, 128), jnp.int32),
            pltpu.SMEM((n_col, 1, 128), jnp.int32),
            dma, dma((n_col,)), dma((n_col,)), dma,
            dma((steps, n_col)), dma((steps, n_col)),
            dma((steps - HALVES, n_row)), dma((steps - HALVES, n_row)),
        ],
        compiler_params=pltpu.CompilerParams(
            collective_id=0, has_side_effects=True, vmem_limit_bytes=60 * 1024 * 1024
        ),
    )(perm, scol, cont, ends, pos, query_ids.reshape(1, queries), damping.reshape(1, queries), tile_block)


def solution(mesh):
    in_specs = (
        P("row", "col", None, None, None),
        P("row", "col", None),
        P("row", "col", None),
        P("row", "col"),
        P(),
        P(),
    )
    out_specs = P(("row", "col"), None)
    return jax.shard_map(shards, mesh=mesh, in_specs=in_specs, out_specs=out_specs, check_vma=False)
```

```python
import functools

import jax
import jax.numpy as jnp
from jax import lax
from jax.experimental import pallas as pl
from jax.experimental.pallas import tpu as pltpu
from jax.sharding import PartitionSpec as P

BPD = 8
TERMS = 4
TOUCH = 4
GROUPS = 4
UNROLL = 32
MESH = pl.DeviceIdType.MESH


def plan(rows, cols, count, n_col, me_col):
    slots = rows.shape[0]
    row_blocks = BPD * n_col
    slot = jnp.arange(slots, dtype=jnp.int32)
    key = jnp.where(slot < count, rows, row_blocks)
    before = (key[None, :] < key[:, None]) | ((key[None, :] == key[:, None]) & (slot[None, :] < slot[:, None]))
    rank = jnp.sum(before.astype(jnp.int32), axis=1)
    at = (rank[None, :] == slot[:, None]).astype(jnp.int32)
    perm = jnp.sum(at * slot[None, :], axis=1)
    scol = jnp.sum(at * cols[None, :], axis=1)
    same = (key[None, :] == key[:, None]) & (slot[None, :] < slot[:, None])
    cont_of = jnp.any(same, axis=1).astype(jnp.int32)
    cont = jnp.sum(at * cont_of[None, :], axis=1)
    blocks = jnp.arange(row_blocks, dtype=jnp.int32)
    hits = key[None, :] == blocks[:, None]
    marked = jnp.any(hits, axis=1).reshape(n_col, BPD)
    last = (jnp.sum((key[None, :] <= blocks[:, None]).astype(jnp.int32), axis=1) - 1).reshape(n_col, BPD)
    local = jnp.arange(BPD, dtype=jnp.int32)
    earlier = marked[:, None, :] & (local[None, None, :] < local[None, :, None])
    place = jnp.sum(earlier.astype(jnp.int32), axis=2)
    places = jnp.arange(TOUCH, dtype=jnp.int32)
    select = marked[:, None, :] & (place[:, None, :] == places[None, :, None])
    ends = jnp.sum(select.astype(jnp.int32) * last[:, None, :], axis=2).reshape(n_col * TOUCH)
    pos = jnp.where(marked, me_col * TOUCH + place, n_col * TOUCH)
    pos = jnp.pad(pos, ((0, 0), (0, 128 - BPD))).reshape(n_col, 1, 128)
    return perm, scol, cont, ends, pos


def katz_kernel(
    n_row, n_col,
    perm, scol, cont, ends,
    pos_ref, qid_ref, damp_ref, tiles_hbm,
    out_ref,
    tiles, run, send, got, xbuf, total, coef, posbuf, pos_smem,
    tile_sem, pos_send, pos_recv, local_sem, send_sem, recv_sem, xsend_sem, xrecv_sem, xpass_sem,
):
    me_r = lax.axis_index("row")
    me_c = lax.axis_index("col")
    slots, tile, _ = tiles.shape
    queries = qid_ref.shape[1]
    width = queries // GROUPS

    load = pltpu.make_async_copy(tiles_hbm, tiles, tile_sem)
    load.start()
    barrier = pltpu.get_barrier_semaphore()
    for d in range(1, n_col):
        pl.semaphore_signal(barrier, inc=1, device_id=(me_r, lax.rem(me_c + d, n_col)), device_id_type=MESH)
    for d in range(1, n_row):
        pl.semaphore_signal(barrier, inc=1, device_id=(lax.rem(me_r + d, n_row), me_c), device_id_type=MESH)

    lane = lax.broadcasted_iota(jnp.int32, (queries, tile), 1)
    qid = jnp.transpose(jnp.broadcast_to(qid_ref[...], (tile, queries))) - lane
    coef[...] = jnp.transpose(jnp.broadcast_to(damp_ref[...], (tile, queries)))

    def first_x(j, carry):
        base = ((j // BPD * n_col + me_c) * BPD + lax.rem(j, BPD)) * tile
        hot = jnp.where(qid == base, 1.0, 0.0).astype(jnp.bfloat16)
        for h in range(GROUPS):
            xbuf[h][j] = hot[h * width:(h + 1) * width]
        return carry

    lax.fori_loop(0, n_row * BPD, first_x, 0)
    for t in range(TERMS * GROUPS):
        got[t][n_col * TOUCH] = jnp.zeros((width, tile), jnp.bfloat16)
    load.wait()

    def compute(t):
        def body(i, acc):
            for u in range(UNROLL):
                p = i * UNROLL + u
                prod = lax.dot_general(
                    xbuf[t][scol[p]], tiles[perm[p]], (((1,), (1,)), ((), ())), preferred_element_type=jnp.float32
                )
                acc = jnp.where(cont[p] > 0, acc, 0.0) + prod
                run[p] = acc.astype(jnp.bfloat16)
            return acc

        lax.fori_loop(0, slots // UNROLL, body, jnp.zeros((width, tile), jnp.float32))

        def pack(s, carry):
            send[t, s] = run[ends[s]]
            return carry

        lax.fori_loop(0, n_col * TOUCH, pack, 0, unroll=4)
        for j in range(TOUCH):
            got[t][me_c * TOUCH + j] = run[ends[me_c * TOUCH + j]]

    def part_copy(t, d):
        peer = lax.rem(me_c + d, n_col)
        return pltpu.make_async_remote_copy(
            src_ref=send.at[t, pl.ds(peer * TOUCH, TOUCH)],
            dst_ref=got[t].at[pl.ds(me_c * TOUCH, TOUCH)],
            send_sem=send_sem.at[t], recv_sem=recv_sem.at[t],
            device_id=(me_r, peer), device_id_type=MESH,
        )

    def all_parts(t):
        every = pl.ds(0, (n_col - 1) * TOUCH)
        return pltpu.make_async_remote_copy(
            src_ref=send.at[t, every], dst_ref=got[t].at[every],
            send_sem=send_sem.at[t], recv_sem=recv_sem.at[t],
            device_id=(me_r, lax.rem(me_c + 1, n_col)), device_id_type=MESH,
        )

    def pos_copy(d):
        peer = lax.rem(me_c + d, n_col)
        return pltpu.make_async_remote_copy(
            src_ref=pos_ref.at[peer], dst_ref=posbuf.at[me_c],
            send_sem=pos_send.at[d], recv_sem=pos_recv.at[d],
            device_id=(me_r, peer), device_id_type=MESH,
        )

    is_end = (me_r == 0) | (me_r == n_row - 1)

    def x_rows(t, first, count, peer, sems, where):
        rows = pl.ds(first * BPD, count * BPD)
        return pltpu.make_async_remote_copy(
            src_ref=xbuf[t + GROUPS].at[rows], dst_ref=xbuf[t + GROUPS].at[rows],
            send_sem=sems.at[t, where], recv_sem=(xpass_sem if where == n_row else xrecv_sem).at[t],
            device_id=(peer, me_c), device_id_type=MESH,
        )

    def for_targets(t, act):
        order = [(lax.rem(me_r + d, n_row), d) for d in (1, n_row - 1, *range(2, n_row - 1))]
        for peer, d in order[:n_row - 1] if n_row > 2 else order[:1]:
            far = jnp.abs(peer - me_r) > 1
            skip = far & ((peer == 0) | (peer == n_row - 1))

            @pl.when(jnp.logical_not(skip))
            def _():
                act(x_rows(t, me_r, 1, peer, xsend_sem, d))

    def for_passes(t, act):
        if n_row > 2:
            @pl.when(me_r == 1)
            def _():
                act(x_rows(t, 2, n_row - 2, 0, xsend_sem, n_row))

            @pl.when(me_r == n_row - 2)
            def _():
                act(x_rows(t, 0, n_row - 2, n_row - 1, xsend_sem, n_row))

    def x_pass(t):
        @pl.when(is_end)
        def _():
            x_rows(t, 0, 1, lax.rem(me_r + 1, n_row), xsend_sem, 0).wait_recv()

        @pl.when(jnp.logical_not(is_end))
        def _():
            x_rows(t, 0, n_row - 1, lax.rem(me_r + 1, n_row), xsend_sem, 0).wait_recv()

        for_passes(t, lambda copy: copy.start())

    def x_ready(t):
        if n_row > 2:
            @pl.when(is_end)
            def _():
                x_rows(t, 0, n_row - 2, lax.rem(me_r + 1, n_row), xsend_sem, n_row).wait_recv()

    def reduce(t):
        k, h = divmod(t, GROUPS)
        all_parts(t).wait_recv()
        part = pl.ds(h * width, width)
        weight = coef[part, :]
        scale = weight
        for _ in range(k - 1):
            scale = scale * weight

        def block(b, carry):
            acc = got[t][pos_smem[0, 0, b]].astype(jnp.float32)
            for s in range(1, n_col):
                acc = acc + got[t][pos_smem[s, 0, b]].astype(jnp.float32)
            if k == 0:
                total[b, part, :] = acc
            else:
                total[b, part, :] = total[b, part, :] + scale * acc
            if k + 1 < TERMS:
                xbuf[t + GROUPS][me_r * BPD + b] = acc.astype(jnp.bfloat16)
            return carry

        lax.fori_loop(0, BPD, block, 0)
        if k + 1 < TERMS:
            for_targets(t, lambda copy: copy.start())

    steps = TERMS * GROUPS
    moves = steps - GROUPS
    for t in range(steps + 1):
        if t < steps:
            if t >= GROUPS:
                x_ready(t - GROUPS)
            compute(t)
            if t == 0:
                pl.semaphore_wait(barrier, n_col - 1 + n_row - 1)
                for d in range(1, n_col):
                    pos_copy(d).start()
            for d in range(1, n_col):
                part_copy(t, d).start()
            if t == 0:
                own = pltpu.make_async_copy(pos_ref.at[me_c], posbuf.at[me_c], local_sem)
                own.start()
                own.wait()
                for d in range(1, n_col):
                    pos_copy(d).wait_recv()
                spill = pltpu.make_async_copy(posbuf, pos_smem, local_sem)
                spill.start()
                spill.wait()
        if t >= 1:
            reduce(t - 1)
        if 2 <= t < moves + 2:
            x_pass(t - 2)

    for b in range(BPD):
        out_ref[pl.ds(b * tile, tile), :] = jnp.transpose(total[b])
    for d in range(1, n_col):
        pos_copy(d).wait_send()
    for t in range(steps):
        all_parts(t).wait_send()
    for t in range(moves):
        for_targets(t, lambda copy: copy.wait_send())
        for_passes(t, lambda copy: copy.wait_send())


def shards(tiles, tile_row, tile_col, tile_count, query_ids, damping):
    tile_block = tiles[0, 0]
    slots, tile, _ = tile_block.shape
    queries = query_ids.shape[0]
    n_row = lax.axis_size("row")
    n_col = lax.axis_size("col")
    me_col = lax.axis_index("col")
    perm, scol, cont, ends, pos = plan(tile_row[0, 0], tile_col[0, 0], tile_count[0, 0], n_col, me_col)
    width = queries // GROUPS
    steps = TERMS * GROUPS
    moves = steps - GROUPS
    bf16 = jnp.bfloat16
    dma = pltpu.SemaphoreType.DMA
    smem = pl.BlockSpec(memory_space=pltpu.SMEM)
    vmem = pl.BlockSpec(memory_space=pltpu.VMEM)
    return pl.pallas_call(
        functools.partial(katz_kernel, n_row, n_col),
        out_shape=jax.ShapeDtypeStruct((BPD * tile, queries), jnp.float32),
        in_specs=[smem] * 4 + [vmem] * 3 + [pl.BlockSpec(memory_space=pl.ANY)],
        out_specs=vmem,
        scratch_shapes=[
            pltpu.VMEM((slots, tile, tile), bf16),
            pltpu.VMEM((slots, width, tile), bf16),
            pltpu.VMEM((steps, n_col * TOUCH, width, tile), bf16),
            [pltpu.VMEM((n_col * TOUCH + 1, width, tile), bf16)] * steps,
            [pltpu.VMEM((n_row * BPD, width, tile), bf16)] * steps,
            pltpu.VMEM((BPD, queries, tile), jnp.float32),
            pltpu.VMEM((queries, tile), jnp.float32),
            pltpu.VMEM((n_col, 1, 128), jnp.int32),
            pltpu.SMEM((n_col, 1, 128), jnp.int32),
            dma, dma((n_col,)), dma((n_col,)), dma,
            dma((steps,)), dma((steps,)),
            dma((moves, n_row + 1)), dma((moves,)), dma((moves,)),
        ],
        compiler_params=pltpu.CompilerParams(
            collective_id=0, has_side_effects=True, vmem_limit_bytes=60 * 1024 * 1024
        ),
    )(perm, scol, cont, ends, pos, query_ids.reshape(1, queries), damping.reshape(1, queries), tile_block)


def solution(mesh):
    in_specs = (
        P("row", "col", None, None, None),
        P("row", "col", None),
        P("row", "col", None),
        P("row", "col"),
        P(),
        P(),
    )
    out_specs = P(("row", "col"), None)
    return jax.shard_map(shards, mesh=mesh, in_specs=in_specs, out_specs=out_specs, check_vma=False)
```

```python
import functools

import jax
import jax.numpy as jnp
from jax import lax
from jax.experimental import pallas as pl
from jax.experimental.pallas import tpu as pltpu
from jax.sharding import PartitionSpec as P

BPD = 8
TERMS = 4
TOUCH = 4
GROUPS = 4
UNROLL = 64
MESH = pl.DeviceIdType.MESH


def plan(rows, cols, count, n_col, me_col):
    slots = rows.shape[0]
    row_blocks = BPD * n_col
    slot = jnp.arange(slots, dtype=jnp.int32)
    key = jnp.where(slot < count, rows, row_blocks)
    before = (key[None, :] < key[:, None]) | ((key[None, :] == key[:, None]) & (slot[None, :] < slot[:, None]))
    rank = jnp.sum(before.astype(jnp.int32), axis=1)
    at = (rank[None, :] == slot[:, None]).astype(jnp.int32)
    perm = jnp.sum(at * slot[None, :], axis=1)
    scol = jnp.sum(at * cols[None, :], axis=1)
    same = (key[None, :] == key[:, None]) & (slot[None, :] < slot[:, None])
    cont_of = jnp.any(same, axis=1).astype(jnp.int32)
    cont = jnp.sum(at * cont_of[None, :], axis=1)
    blocks = jnp.arange(row_blocks, dtype=jnp.int32)
    hits = key[None, :] == blocks[:, None]
    marked = jnp.any(hits, axis=1).reshape(n_col, BPD)
    last = (jnp.sum((key[None, :] <= blocks[:, None]).astype(jnp.int32), axis=1) - 1).reshape(n_col, BPD)
    local = jnp.arange(BPD, dtype=jnp.int32)
    earlier = marked[:, None, :] & (local[None, None, :] < local[None, :, None])
    place = jnp.sum(earlier.astype(jnp.int32), axis=2)
    places = jnp.arange(TOUCH, dtype=jnp.int32)
    select = marked[:, None, :] & (place[:, None, :] == places[None, :, None])
    ends = jnp.sum(select.astype(jnp.int32) * last[:, None, :], axis=2).reshape(n_col * TOUCH)
    pos = jnp.where(marked, me_col * TOUCH + place, n_col * TOUCH)
    pos = jnp.pad(pos, ((0, 0), (0, 128 - BPD))).reshape(n_col, 1, 128)
    return perm, scol, cont, ends, pos


def katz_kernel(
    n_row, n_col,
    perm, scol, cont, ends,
    pos_ref, qid_ref, damp_ref, tiles_hbm,
    out_ref,
    tiles, flip, run, send, got, xbuf, total, coef, posbuf, pos_smem,
    tile_sem, pos_send, pos_recv, local_sem, send_sem, recv_sem, xsend_sem, xrecv_sem, xpass_sem,
):
    me_r = lax.axis_index("row")
    me_c = lax.axis_index("col")
    slots, tile, _ = tiles.shape
    queries = qid_ref.shape[1]
    width = queries // GROUPS

    load = pltpu.make_async_copy(tiles_hbm, tiles, tile_sem)
    load.start()
    barrier = pltpu.get_barrier_semaphore()
    for d in range(1, n_col):
        pl.semaphore_signal(barrier, inc=1, device_id=(me_r, lax.rem(me_c + d, n_col)), device_id_type=MESH)
    for d in range(1, n_row):
        pl.semaphore_signal(barrier, inc=1, device_id=(lax.rem(me_r + d, n_row), me_c), device_id_type=MESH)

    lane = lax.broadcasted_iota(jnp.int32, (queries, tile), 1)
    qid = jnp.transpose(jnp.broadcast_to(qid_ref[...], (tile, queries))) - lane
    coef[...] = jnp.transpose(jnp.broadcast_to(damp_ref[...], (tile, queries)))

    def first_x(j, carry):
        base = ((j // BPD * n_col + me_c) * BPD + lax.rem(j, BPD)) * tile
        hot = jnp.where(qid == base, 1.0, 0.0).astype(jnp.bfloat16)
        for h in range(GROUPS):
            xbuf[h][j] = hot[h * width:(h + 1) * width]
        return carry

    lax.fori_loop(0, n_row * BPD, first_x, 0)
    for t in range(TERMS * GROUPS):
        got[t][n_col * TOUCH] = jnp.zeros((width, tile), jnp.bfloat16)
    load.wait()

    def compute(t):
        def body(i, acc):
            for u in range(0, UNROLL, 2):
                p = i * UNROLL + u
                if t == 0:
                    flip[p // 2, :, :tile] = jnp.transpose(tiles[perm[p]])
                    flip[p // 2, :, tile:] = jnp.transpose(tiles[perm[p + 1]])
                both = jnp.concatenate([xbuf[t][scol[p]], xbuf[t][scol[p + 1]]], axis=0)
                prod = jnp.dot(both, flip[p // 2], preferred_element_type=jnp.float32)
                acc = jnp.where(cont[p] > 0, acc, 0.0) + prod[:width, :tile]
                run[p] = acc.astype(jnp.bfloat16)
                acc = jnp.where(cont[p + 1] > 0, acc, 0.0) + prod[width:, tile:]
                run[p + 1] = acc.astype(jnp.bfloat16)
            return acc

        lax.fori_loop(0, slots // UNROLL, body, jnp.zeros((width, tile), jnp.float32))

        def pack(s, carry):
            send[t, s] = run[ends[s]]
            return carry

        lax.fori_loop(0, n_col * TOUCH, pack, 0, unroll=n_col * TOUCH)
        for j in range(TOUCH):
            got[t][me_c * TOUCH + j] = run[ends[me_c * TOUCH + j]]

    def part_copy(t, d):
        peer = lax.rem(me_c + d, n_col)
        return pltpu.make_async_remote_copy(
            src_ref=send.at[t, pl.ds(peer * TOUCH, TOUCH)],
            dst_ref=got[t].at[pl.ds(me_c * TOUCH, TOUCH)],
            send_sem=send_sem.at[t], recv_sem=recv_sem.at[t],
            device_id=(me_r, peer), device_id_type=MESH,
        )

    def all_parts(t):
        every = pl.ds(0, (n_col - 1) * TOUCH)
        return pltpu.make_async_remote_copy(
            src_ref=send.at[t, every], dst_ref=got[t].at[every],
            send_sem=send_sem.at[t], recv_sem=recv_sem.at[t],
            device_id=(me_r, lax.rem(me_c + 1, n_col)), device_id_type=MESH,
        )

    def pos_copy(d):
        peer = lax.rem(me_c + d, n_col)
        return pltpu.make_async_remote_copy(
            src_ref=pos_ref.at[peer], dst_ref=posbuf.at[me_c],
            send_sem=pos_send.at[d], recv_sem=pos_recv.at[d],
            device_id=(me_r, peer), device_id_type=MESH,
        )

    is_end = (me_r == 0) | (me_r == n_row - 1)

    def x_rows(t, first, count, peer, sems, where):
        rows = pl.ds(first * BPD, count * BPD)
        return pltpu.make_async_remote_copy(
            src_ref=xbuf[t + GROUPS].at[rows], dst_ref=xbuf[t + GROUPS].at[rows],
            send_sem=sems.at[t, where], recv_sem=(xpass_sem if where == n_row else xrecv_sem).at[t],
            device_id=(peer, me_c), device_id_type=MESH,
        )

    def for_targets(t, act):
        order = [(lax.rem(me_r + d, n_row), d) for d in (1, n_row - 1, *range(2, n_row - 1))]
        for peer, d in order[:n_row - 1] if n_row > 2 else order[:1]:
            far = jnp.abs(peer - me_r) > 1
            skip = far & ((peer == 0) | (peer == n_row - 1))

            @pl.when(jnp.logical_not(skip))
            def _():
                act(x_rows(t, me_r, 1, peer, xsend_sem, d))

    def for_passes(t, act):
        if n_row > 2:
            @pl.when(me_r == 1)
            def _():
                act(x_rows(t, 2, n_row - 2, 0, xsend_sem, n_row))

            @pl.when(me_r == n_row - 2)
            def _():
                act(x_rows(t, 0, n_row - 2, n_row - 1, xsend_sem, n_row))

    def x_pass(t):
        @pl.when(is_end)
        def _():
            x_rows(t, 0, 1, lax.rem(me_r + 1, n_row), xsend_sem, 0).wait_recv()

        @pl.when(jnp.logical_not(is_end))
        def _():
            x_rows(t, 0, n_row - 1, lax.rem(me_r + 1, n_row), xsend_sem, 0).wait_recv()

        for_passes(t, lambda copy: copy.start())

    def x_ready(t):
        if n_row > 2:
            @pl.when(is_end)
            def _():
                x_rows(t, 0, n_row - 2, lax.rem(me_r + 1, n_row), xsend_sem, n_row).wait_recv()

    def reduce(t):
        k, h = divmod(t, GROUPS)
        all_parts(t).wait_recv()
        part = pl.ds(h * width, width)
        weight = coef[part, :]
        scale = weight
        for _ in range(k - 1):
            scale = scale * weight

        def block(b, carry):
            acc = got[t][pos_smem[0, 0, b]].astype(jnp.float32)
            for s in range(1, n_col):
                acc = acc + got[t][pos_smem[s, 0, b]].astype(jnp.float32)
            if k == 0:
                total[b, part, :] = acc
            else:
                total[b, part, :] = total[b, part, :] + scale * acc
            if k + 1 < TERMS:
                xbuf[t + GROUPS][me_r * BPD + b] = acc.astype(jnp.bfloat16)
            return carry

        lax.fori_loop(0, BPD, block, 0, unroll=BPD)
        if k + 1 < TERMS:
            for_targets(t, lambda copy: copy.start())

    steps = TERMS * GROUPS
    moves = steps - GROUPS
    for t in range(steps + 1):
        if t < steps:
            if t >= GROUPS:
                x_ready(t - GROUPS)
            compute(t)
            if t == 0:
                pl.semaphore_wait(barrier, n_col - 1 + n_row - 1)
                for d in range(1, n_col):
                    pos_copy(d).start()
            for d in range(1, n_col):
                part_copy(t, d).start()
            if t == 1:
                own = pltpu.make_async_copy(pos_ref.at[me_c], posbuf.at[me_c], local_sem)
                own.start()
                own.wait()
                for d in range(1, n_col):
                    pos_copy(d).wait_recv()
                spill = pltpu.make_async_copy(posbuf, pos_smem, local_sem)
                spill.start()
                spill.wait()
        if t >= 1:
            reduce(t - 1)
        if 2 <= t < moves + 2:
            x_pass(t - 2)

    for b in range(BPD):
        out_ref[pl.ds(b * tile, tile), :] = jnp.transpose(total[b])
    for d in range(1, n_col):
        pos_copy(d).wait_send()
    for t in range(steps):
        all_parts(t).wait_send()
    for t in range(moves):
        for_targets(t, lambda copy: copy.wait_send())
        for_passes(t, lambda copy: copy.wait_send())


def shards(tiles, tile_row, tile_col, tile_count, query_ids, damping):
    tile_block = tiles[0, 0]
    slots, tile, _ = tile_block.shape
    queries = query_ids.shape[0]
    n_row = lax.axis_size("row")
    n_col = lax.axis_size("col")
    me_col = lax.axis_index("col")
    perm, scol, cont, ends, pos = plan(tile_row[0, 0], tile_col[0, 0], tile_count[0, 0], n_col, me_col)
    width = queries // GROUPS
    steps = TERMS * GROUPS
    moves = steps - GROUPS
    bf16 = jnp.bfloat16
    dma = pltpu.SemaphoreType.DMA
    smem = pl.BlockSpec(memory_space=pltpu.SMEM)
    vmem = pl.BlockSpec(memory_space=pltpu.VMEM)
    return pl.pallas_call(
        functools.partial(katz_kernel, n_row, n_col),
        out_shape=jax.ShapeDtypeStruct((BPD * tile, queries), jnp.float32),
        in_specs=[smem] * 4 + [vmem] * 3 + [pl.BlockSpec(memory_space=pl.ANY)],
        out_specs=vmem,
        scratch_shapes=[
            pltpu.VMEM((slots, tile, tile), bf16),
            pltpu.VMEM((slots // 2, tile, 2 * tile), bf16),
            pltpu.VMEM((slots, width, tile), bf16),
            pltpu.VMEM((steps, n_col * TOUCH, width, tile), bf16),
            [pltpu.VMEM((n_col * TOUCH + 1, width, tile), bf16)] * steps,
            [pltpu.VMEM((n_row * BPD, width, tile), bf16)] * steps,
            pltpu.VMEM((BPD, queries, tile), jnp.float32),
            pltpu.VMEM((queries, tile), jnp.float32),
            pltpu.VMEM((n_col, 1, 128), jnp.int32),
            pltpu.SMEM((n_col, 1, 128), jnp.int32),
            dma, dma((n_col,)), dma((n_col,)), dma,
            dma((steps,)), dma((steps,)),
            dma((moves, n_row + 1)), dma((moves,)), dma((moves,)),
        ],
        compiler_params=pltpu.CompilerParams(
            collective_id=0, has_side_effects=True, vmem_limit_bytes=60 * 1024 * 1024
        ),
    )(perm, scol, cont, ends, pos, query_ids.reshape(1, queries), damping.reshape(1, queries), tile_block)


def solution(mesh):
    in_specs = (
        P("row", "col", None, None, None),
        P("row", "col", None),
        P("row", "col", None),
        P("row", "col"),
        P(),
        P(),
    )
    out_specs = P(("row", "col"), None)
    return jax.shard_map(shards, mesh=mesh, in_specs=in_specs, out_specs=out_specs, check_vma=False)
```
